32 devices in a mesh: au: 8 (over z, core), vert: 4 (over y, x).
Axes of the slice: x: 2, y: 2, z: 4, core: 2. Of those that a mesh axis runs over, the one named last changes fastest.
Arguments:
- vis_value: float32 [128, 128, 2, 128], P('au', 'vert'), may hold values from -6 to 6
- vis_pos: int32 [128, 128, 2, 128], P('au', 'vert'), may hold values from 0 to 1048575, as said below
- counts: int32 [128, 128], P('au', 'vert'), may hold values from 21 to 128, as said below
- kernel: float32 [8, 128], replicated, may hold values from 0.05 to 0.5
Outputs:
- image: float32 [8192, 8192], P(('au', 'vert'))
The draws below stay inside these ranges and needn't reach their ends.
Inputs may be any that keep to these rules, and one draw needn't show every extreme that they name: Slot k of patch (p, q) holds a visibility exactly when k < counts[p, q]; in every draw some patch has all 128 slots live. vis_pos[p, q, 0, k] lies in [p * 64 * 128, (p + 1) * 64 * 128) and vis_pos[p, q, 1, k] in [q * 64 * 128, (q + 1) * 64 * 128), in every slot.
All inputs are finite; a program needn't handle non-finite values.
Results may differ from the reference program's by a relative error of at most 0.0003.
Values sent between devices are 32-bit elements; how exact they have to be, the bound alone decides.
A program may use at most 192 MiB of HBM per device.

```python
import math
import jax
import jax.numpy as jnp
from jax import lax

PATCH = 64
KW = 8
OVER = 128
PR = 128
PCAP = 128
PC = 128


def draw_vis_pos(key, part):
    local_fine = jax.random.randint(key, (PR, PC, 2, PCAP), 0, PATCH * OVER, dtype=jnp.int32)
    row_index = jnp.arange(PR, dtype=jnp.int32)[:, None, None, None]
    col_index = jnp.arange(PC, dtype=jnp.int32)[None, :, None, None]
    component = jnp.arange(2, dtype=jnp.int32)[None, None, :, None]
    patch_base = jnp.where(component == 0, row_index, col_index) * (PATCH * OVER)
    return patch_base + local_fine


def draw_counts(key, part):
    key_counts, key_row, key_col = jax.random.split(jax.random.fold_in(key, 7), 3)
    radius = max(PR // 2, 1)
    row_index = jnp.arange(PR, dtype=jnp.int32)[:, None]
    col_index = jnp.arange(PC, dtype=jnp.int32)[None, :]
    cycle_index = jnp.maximum(jnp.abs(2 * row_index + 1 - PR), jnp.abs(2 * col_index + 1 - PC)) // 2
    scaled = cycle_index * 64 // radius
    ceiling = PCAP * 32 // (32 + scaled)
    drawn_counts = jax.random.randint(key_counts, (PR, PC), ceiling // 2, ceiling + 1, dtype=jnp.int32)
    chosen_row = jax.random.randint(key_row, (), 0, PR, dtype=jnp.int32)
    chosen_col = jax.random.randint(key_col, (), 0, PC, dtype=jnp.int32)
    full_patch = (row_index == chosen_row) & (col_index == chosen_col)
    return jnp.where(full_patch, PCAP, drawn_counts).astype(jnp.int32)


def shard_levels(rng, dims, cuts, least, largest):
    loudness = 1.0
    for position, parts in cuts:
        steps = jax.random.uniform(jax.random.fold_in(jax.random.fold_in(rng, 6), position), (parts,), jnp.float32, least / len(cuts), largest / len(cuts))
        loudness = loudness * jnp.repeat(jnp.exp(steps), dims[position] // parts).reshape((-1,) + (1,) * (len(dims) - 1 - position))
    return loudness


def scatter_about(key, dims, deviation, reach, pieces=(), held_as=jnp.bfloat16):
    result = jax.random.normal(key, dims, jnp.float32) * deviation
    if len(pieces) > 0:
        result = shard_levels(key, dims, pieces, -0.22, 0.18) * result
    return jnp.clip(result, min=-reach, max=reach).astype(held_as)


def setup_inputs(seed: int = 0) -> dict:
    key_of = jax.random.split(jax.random.key(seed), 5)
    vis_value = scatter_about(key_of[0], (PR, PC, 2, PCAP), 1.0, 6.0, ((0, 8), (1, 4)), jnp.float32)
    vis_pos = draw_vis_pos(jax.random.fold_in(key_of[4], 71), 0)
    counts = draw_counts(jax.random.fold_in(key_of[4], 71), 0)
    kernel = jnp.clip(jax.random.uniform(key_of[3], (KW, OVER), jnp.float32, 0.05, 0.5), 0.05, 0.5)
    return {"vis_value": vis_value, "vis_pos": vis_pos, "counts": counts, "kernel": kernel}


def reference(vis_value, vis_pos, counts, kernel):
    kernel_width, oversample = kernel.shape
    grid_size = PR * PATCH
    extent = PATCH + kernel_width
    slot_count = vis_value.shape[3]
    tap_table = kernel.T

    def one_row(pending, row_number):
        values = lax.dynamic_index_in_dim(vis_value, row_number, 0, keepdims=False)
        positions = lax.dynamic_index_in_dim(vis_pos, row_number, 0, keepdims=False)
        tallies = lax.dynamic_index_in_dim(counts, row_number, 0, keepdims=False)
        cell_index = positions // oversample
        fine_index = positions - cell_index * oversample
        offsets = cell_index % PATCH
        tap_values = tap_table[fine_index]
        live_mask = (jnp.arange(slot_count, dtype=jnp.int32)[None, :] < tallies[:, None]).astype(jnp.float32)
        distance = jnp.arange(extent, dtype=jnp.int32)[None, None, None, :] - offsets[..., None]
        weights = jnp.zeros(distance.shape, jnp.float32)
        for tap_step in range(kernel_width):
            weights = weights + jnp.where(distance == tap_step, tap_values[..., tap_step:tap_step + 1], 0.0)
        row_weights = weights[:, 0] * live_mask[:, :, None]
        scaled = values[:, :, :, None] * weights[:, 1][:, None]
        patches = jnp.einsum('nki,nckj->ncij', row_weights, scaled, precision=lax.Precision.HIGHEST)
        core_part = patches[..., :PATCH].transpose(1, 2, 0, 3)
        spill_cols = jnp.pad(patches[..., PATCH:].transpose(1, 2, 0, 3), ((0, 0), (0, 0), (0, 0), (0, PATCH - kernel_width)))
        band_field = jnp.pad(core_part, ((0, 0), (0, 0), (0, 1), (0, 0))) + jnp.pad(spill_cols, ((0, 0), (0, 0), (1, 0), (0, 0)))
        band_field = band_field.reshape(2, extent, (PC + 1) * PATCH)[:, :, :grid_size]
        band_field = band_field.at[:, :kernel_width].add(pending)
        finished = band_field[:, :PATCH]
        complex_rows = finished[0] + 1j * finished[1]
        spectrum = jnp.fft.ifft(complex_rows, axis=1) * grid_size
        return (band_field[:, PATCH:], spectrum)
    start_rim = jnp.zeros((2, kernel_width, grid_size), jnp.float32)
    _, spectra = lax.scan(one_row, start_rim, jnp.arange(PR, dtype=jnp.int32))
    spectra = spectra.reshape(grid_size, grid_size)
    block_size = min(512, grid_size)
    image_scale = 1.0 / math.sqrt(PR * PC * slot_count)

    def one_block(offset_start):
        column_block = lax.dynamic_slice_in_dim(spectra, offset_start, block_size, 1)
        return ((jnp.fft.ifft(column_block, axis=0) * grid_size).real.T * image_scale).astype(jnp.float32)
    images = lax.map(one_block, jnp.arange(grid_size // block_size, dtype=jnp.int32) * block_size)
    return images.reshape(grid_size, grid_size)
```

```python
import functools
import math

import jax
import jax.numpy as jnp
from jax import lax
from jax.experimental import pallas as pl
from jax.experimental.pallas import tpu as pltpu
from jax.sharding import Mesh, PartitionSpec as P

PATCH = 64
LANES = 128
SUB = 8

BF16 = jnp.bfloat16
F32 = jnp.float32


def split(x):
    hi = x.astype(BF16)
    lo = (x - hi.astype(F32)).astype(BF16)
    return hi, lo


def dot(lhs, rhs):
    return lax.dot_general(lhs, rhs, (((1,), (0,)), ((), ())), preferred_element_type=F32)


def dot_nt(lhs, rhs):
    return lax.dot_general(lhs, rhs, (((1,), (1,)), ((), ())), preferred_element_type=F32)


def turn(product, length):
    angle = (2.0 * math.pi / length) * (product % length).astype(F32)
    return jnp.cos(angle), jnp.sin(angle)


def real_parts(cos, sin):
    return jnp.stack([jnp.stack([cos, -sin]), jnp.stack([sin, cos])])


def tap_blocks(kern, cells, base, mirrored, length, wrap):
    slots = cells.shape[1]
    shape = (SUB, slots)
    cell = lax.shift_right_logical(cells, 7)
    fine = jnp.broadcast_to(cells & 127, shape)
    taps = jnp.take_along_axis(kern, fine, axis=1, mode="promise_in_bounds")
    sub = lax.broadcasted_iota(jnp.int32, shape, 0)
    taps = jnp.where(jnp.broadcast_to(cell, shape) + sub < length, taps, 0.0)
    off = jnp.broadcast_to(cell & (PATCH - 1), shape)
    if mirrored:
        place = base + PATCH - off
        tap = (place - sub) & (SUB - 1)
        block = lax.shift_right_arithmetic(place - tap, 3)
    else:
        place = base + off
        tap = (sub - place) & (SUB - 1)
        block = lax.shift_right_arithmetic(place + tap, 3)
    if wrap:
        block = block & (wrap - 1)
    turned = jnp.take_along_axis(taps, tap, axis=0, mode="promise_in_bounds")
    return turned, block


def patch_operands(kern, fields, mirrored, parity, length):
    values_re, values_im = fields[0:1], fields[1:2]
    cells = fields[2:4].astype(jnp.int32)
    rows, row_block = tap_blocks(kern, cells[0:1], SUB, mirrored, length, 0)
    cols, col_block = tap_blocks(kern, cells[1:2], PATCH * parity, mirrored, length, 2 * PATCH // SUB)
    if mirrored:
        values_im = -values_im

    def halves(x):
        hi = x.astype(BF16).astype(F32)
        return hi, x - hi

    row_hi, row_lo = halves(rows)
    row_masks = [row_block == j for j in range(PATCH // SUB + 2)]
    a_hi = jnp.concatenate([jnp.where(m, row_hi, 0.0) for m in row_masks], axis=0).astype(BF16)
    a_lo = jnp.concatenate([jnp.where(m, row_lo, 0.0) for m in row_masks], axis=0).astype(BF16)
    col_masks = [col_block == j for j in range(2 * PATCH // SUB)]
    live = [(j - parity * (PATCH // SUB)) % len(col_masks) in (*range(9), 15) for j in range(len(col_masks))]
    zero = jnp.zeros_like(cols)
    b_hi, b_lo = [], []
    for value in (values_re, values_im):
        hi, lo = halves(cols * value)
        b_hi += [jnp.where(m, hi, 0.0) if on else zero for m, on in zip(col_masks, live)]
        b_lo += [jnp.where(m, lo, 0.0) if on else zero for m, on in zip(col_masks, live)]
    return a_hi, a_lo, jnp.concatenate(b_hi, axis=0).astype(BF16), jnp.concatenate(b_lo, axis=0).astype(BF16)


def tile_of(kern, low, high, parity, length):
    la_hi, la_lo, lb_hi, lb_lo = patch_operands(kern, low, False, parity, length)
    ha_hi, ha_lo, hb_hi, hb_lo = patch_operands(kern, high, True, parity, length)
    a_hi = jnp.concatenate([la_hi, ha_hi], axis=1)
    a_lo = jnp.concatenate([la_lo, ha_lo], axis=1)
    b_hi = jnp.concatenate([lb_hi, hb_hi], axis=1)
    b_lo = jnp.concatenate([lb_lo, hb_lo], axis=1)
    rows = a_hi.shape[0]
    main = dot_nt(jnp.concatenate([a_hi, a_lo], axis=0), b_hi)
    return main[:rows] + main[rows:] + dot_nt(a_hi, b_lo)


def grid_kernel(dims, flags_ref, own_ref, par_ref, kern_ref, f1_ref, tw_ref, eh_ref, el_ref, h_ref, g_ref, carry_ref):
    bands, pairs, row_stride, length = dims
    tile_rows = PATCH + 2 * SUB
    is_low = flags_ref[0] == 1
    is_last = flags_ref[1] == 1
    kern = kern_ref[...]
    parts = 2 * pairs
    lane = lax.broadcasted_iota(jnp.int32, (tile_rows, 2 * LANES), 1) & (LANES - 1)

    def clear(n, _):
        for part in range(2):
            base = pl.multiple_of((part * pairs + n) * row_stride, SUB)
            g_ref[pl.ds(base, row_stride), :] = jnp.zeros((row_stride, LANES), F32)
        return 0

    lax.fori_loop(0, pairs, clear, 0)

    for band in range(bands):

        def fields_at(q, parity):
            own_low = own_ref[band, q, 4 * parity : 4 * parity + 4, :]
            par_low = par_ref[band, q, 4 * parity : 4 * parity + 4, :]
            mq = pairs - 1 - q
            mp = 1 - parity
            own_high = own_ref[bands - 1 - band, mq, 4 * mp : 4 * mp + 4, :]
            par_high = par_ref[bands - 1 - band, mq, 4 * mp : 4 * mp + 4, :]
            return jnp.where(is_low, own_low, par_low), jnp.where(is_low, par_high, own_high)

        def columns(q):
            odd = tile_of(kern, *fields_at(q, 1), 1, length)
            nxt = jnp.where(q == pairs - 1, 0, q + 1)
            even = tile_of(kern, *fields_at(nxt, 0), 0, length)
            here = jnp.where(lane < SUB, 0.0, odd) + jnp.where(lane < LANES - SUB, 0.0, even)
            there = jnp.where(lane < SUB, odd, 0.0) + jnp.where(lane < LANES - SUB, even, 0.0)
            return here, there

        _, there = columns(pairs - 1)
        carry_ref[...] = there

        def step(q, _):
            here, there = columns(q)
            total = here + carry_ref[...]
            carry_ref[...] = there
            for part in range(2):
                base = pl.multiple_of((part * pairs + q) * row_stride, SUB) + band * PATCH
                where = pl.ds(base, tile_rows)
                g_ref[where, :] = g_ref[where, :] + total[:, part * LANES : (part + 1) * LANES]
            return 0

        lax.fori_loop(0, pairs, step, 0)

        cos = tw_ref[0]
        sin = tw_ref[1]

        def quad(group, _):
            first = band * PATCH + 4 * group
            lines = []
            for pair in range(2):
                cells = []
                for one in range(2):
                    row = first + 2 * pair + one
                    up = bands * PATCH + SUB
                    j = row - up
                    moved = jnp.where(j == 6, 0, jnp.where(j == 7, 7, jnp.where(j % 2 == 0, j + 2, j)))
                    row = jnp.where(is_last & (j >= 0), up + moved, row)
                    cells.append(g_ref[pl.ds(row, parts, stride=row_stride), :])
                hi, lo = split(jnp.concatenate(cells, axis=1))
                out = dot(f1_ref[...], jnp.concatenate([hi, lo], axis=0))
                out = out[:parts] + out[parts:]
                for one in range(2):
                    re = out[:pairs, one * LANES : (one + 1) * LANES]
                    im = out[pairs:, one * LANES : (one + 1) * LANES]
                    lines.append(jnp.concatenate([re * cos - im * sin, re * sin + im * cos], axis=1))
            hi, lo = split(jnp.concatenate(lines, axis=0))
            count = el_ref.shape[0]
            out = dot_nt(eh_ref[...], hi)
            out = out[:count] + out[count:] + dot_nt(el_ref[...], lo)
            dests, _, share, _ = h_ref.shape
            for part in range(2):
                piece = out[:, part * LANES : (part + 1) * LANES].reshape(dests, share, LANES)
                h_ref[:, first // 2 + part, :, :] = piece
            return 0

        groups = PATCH // 4 + (2 * SUB // 4 if band == bands - 1 else 0)
        lax.fori_loop(0, groups, quad, 0)


def grid_and_rows(flags, own, par, kern, f1, tw, eh, el, dests, length):
    bands, pairs = own.shape[0], own.shape[1]
    rows = bands * PATCH + 2 * SUB
    row_stride = rows + SUB
    outs = el.shape[0]
    vmem = pl.BlockSpec(memory_space=pltpu.VMEM)
    return pl.pallas_call(
        functools.partial(grid_kernel, (bands, pairs, row_stride, length)),
        out_shape=jax.ShapeDtypeStruct((dests, rows * pairs // LANES, outs // dests, LANES), F32),
        in_specs=[pl.BlockSpec(memory_space=pltpu.SMEM)] + [vmem] * 7,
        out_specs=vmem,
        scratch_shapes=[
            pltpu.VMEM((2 * pairs * row_stride, LANES), F32),
            pltpu.VMEM((PATCH + 2 * SUB, 2 * LANES), F32),
        ],
        compiler_params=pltpu.CompilerParams(vmem_limit_bytes=60 * 1024 * 1024),
        name="grid_rows",
    )(flags, own, par, kern, f1, tw, eh, el)


def column_kernel(dims, flags_ref, h_ref, f2_ref, f2l_ref, tw_ref, e2_ref, out_ref, r_ref, z_ref, s_ref, sems):
    sources, spans, bands, block_rows = dims
    share = 2 * spans
    low = flags_ref[0] == 1
    width = LANES
    y_count = spans * PATCH
    half = PATCH // 2

    blocks = h_ref.shape[1]
    stride = (blocks + 1) * share

    @pl.when(pl.program_id(0) == 0)
    def _():
        copies = [
            pltpu.make_async_copy(h_ref.at[n], r_ref.at[pl.ds(n * (blocks + 1), blocks)], sems.at[n])
            for n in range(sources)
        ]
        for copy in copies:
            copy.start()
        for copy in copies:
            copy.wait()
        flat = r_ref.reshape(sources * stride, width)
        up_block = SUB // 2 + bands * half
        sub = lax.broadcasted_iota(jnp.int32, (share, width), 0)
        sign = jnp.where(sub % 2 == 0, 1.0, -1.0)

        def at_block(n, block):
            source = jnp.where(low, n, sources - 1 - n)
            return source * (blocks + 1) + block

        def add(to, value):
            r_ref[to] = r_ref[to] + value

        def neighbours(n, _):
            for t in range(SUB // 2):
                add(at_block(n + 1, SUB // 2 + t), r_ref[at_block(n, up_block + t)])
                add(at_block(n, up_block - SUB // 2 + t), r_ref[at_block(n + 1, t)])
            return 0

        lax.fori_loop(0, sources - 1, neighbours, 0)
        for t in range(SUB // 2 - 1):
            add(at_block(sources - 1, up_block - 1 - t), sign * r_ref[at_block(sources - 1, up_block + t)])
        top = r_ref[at_block(sources - 1, up_block + SUB // 2 - 1)]
        lane = lax.broadcasted_iota(jnp.int32, (share, width), 1)
        lifted = jnp.concatenate([top[share - 1 :], top[: share - 1]], axis=0)
        first = at_block(0, SUB // 2)
        r_ref[first] = jnp.where((sub % 2 == 1) & (lane < PATCH), lifted, r_ref[first])

        odd = lax.broadcasted_iota(jnp.int32, (PATCH, width), 1) % 2
        flip = jnp.where(odd == 0, 1.0, -1.0)

        def pair_step(rho, _):
            tall = []
            for k in range(spans):
                cells = []
                for c in range(2):
                    for i in range(bands):
                        row = (SUB // 2 + i * half + rho) * share + 2 * k + c
                        cells.append(flat[pl.ds(row, sources, stride=stride), :])
                tall.append(jnp.concatenate(cells, axis=0).T)
            x = jnp.concatenate(tall, axis=0)
            hi, lo = split(x)
            z = dot(jnp.concatenate([hi, lo], axis=1), f2_ref[...]) + dot(hi, f2l_ref[...])
            top_col = jnp.where(low, x[:, PATCH : PATCH + 1], x[:, PATCH + sources - 1 : PATCH + sources])
            for k in range(spans):
                for one in range(2):
                    at = (2 * k + one) * PATCH
                    re = z[at : at + PATCH, :width]
                    im = z[at : at + PATCH, width:]
                    line = 2 * rho + one
                    cos = tw_ref[0, pl.ds(line, 1), :]
                    sin = tw_ref[1, pl.ds(line, 1), :]
                    new_re = re * cos - im * sin
                    new_im = re * sin + im * cos
                    if one == 0:
                        nyquist = flip * top_col[at : at + PATCH]
                        new_im = jnp.where(rho == 0, nyquist, new_im)
                    z_ref[pl.ds(pl.multiple_of(line * y_count + k * PATCH, PATCH), PATCH), :] = new_re
                    z_ref[pl.ds(pl.multiple_of((PATCH + line) * y_count + k * PATCH, PATCH), PATCH), :] = new_im
            return 0

        lax.fori_loop(0, half, pair_step, 0)

    start = pl.program_id(0) * block_rows

    def eight(group, _):
        for pair in range(SUB // 2):
            y = start + group * SUB + 2 * pair
            cells = [z_ref[pl.ds(y + one, 2 * PATCH, stride=y_count), :] for one in range(2)]
            hi, lo = split(jnp.concatenate(cells, axis=1))
            out = dot(e2_ref[...], jnp.concatenate([hi, lo], axis=0))
            out = out[:PATCH] + out[PATCH:]
            for one in range(2):
                s_ref[pl.ds(2 * pair + one, PATCH, stride=SUB), :] = out[:, one * width : (one + 1) * width]
        at = pl.ds(pl.multiple_of(group * SUB, SUB), SUB)
        for block in range(PATCH):
            out_ref[at, block * width : (block + 1) * width] = s_ref[block * SUB : (block + 1) * SUB, :]
        return 0

    lax.fori_loop(0, block_rows // SUB, eight, 0)


def columns_of(flags, h, f2, f2l, tw, e2, sources, spans, bands, length):
    y_count = spans * PATCH
    block_rows = min(32, y_count)
    vmem = pl.BlockSpec(memory_space=pltpu.VMEM)
    return pl.pallas_call(
        functools.partial(column_kernel, (sources, spans, bands, block_rows)),
        grid=(y_count // block_rows,),
        out_shape=jax.ShapeDtypeStruct((y_count, length), F32),
        in_specs=[pl.BlockSpec(memory_space=pltpu.SMEM), pl.BlockSpec(memory_space=pl.ANY)] + [vmem] * 4,
        out_specs=pl.BlockSpec((block_rows, length), lambda n: (n, 0)),
        scratch_shapes=[
            pltpu.VMEM((sources * (h.shape[1] + 1), h.shape[2], LANES), F32),
            pltpu.VMEM((2 * PATCH * y_count, LANES), F32),
            pltpu.VMEM((PATCH * SUB, LANES), F32),
            pltpu.SemaphoreType.DMA((sources,)),
        ],
        compiler_params=pltpu.CompilerParams(vmem_limit_bytes=60 * 1024 * 1024),
        name="columns",
    )(flags, h, f2, f2l, tw, e2)


def split_table(x):
    rounded = lax.reduce_precision(x, 8, 7)
    return rounded.astype(BF16), (x - rounded).astype(BF16)


def stacked(table):
    hi, lo = split_table(table)
    return jnp.concatenate([jnp.concatenate([hi, hi], axis=1), jnp.concatenate([lo, jnp.zeros_like(lo)], axis=1)], axis=0)


def local(vis_value, vis_pos, counts, kernel, *, au, vert):
    devices = au * vert
    half_au = au // 2
    axes = ("half", "sub", "vert")
    me = lax.axis_index(axes)
    low = me < devices // 2
    slots = vis_value.shape[3]
    bands = vis_value.shape[0] // vert
    local_cols = vis_value.shape[1]
    cols = local_cols * vert
    pairs = cols // 2
    length = cols * PATCH
    rows_of_patches = vis_value.shape[0] * au
    scale = 1.0 / math.sqrt(rows_of_patches * cols * slots)
    sources = devices // 2
    y_count = length // devices
    spans = y_count // PATCH

    live = jnp.arange(slots, dtype=jnp.int32) < counts[:, :, None, None]
    fields = jnp.concatenate([jnp.where(live, vis_value, 0.0), vis_pos.astype(F32)], axis=2)
    fields = fields.reshape(vert, bands, local_cols // 2, 8, slots)
    own = lax.all_to_all(fields, "vert", split_axis=0, concat_axis=2, tiled=True)
    own = own.reshape(bands, pairs, 8, slots)
    par = lax.ppermute(own, axes, [(d, devices - 1 - d) for d in range(devices)])

    band_index = jnp.where(low, me, devices - 1 - me)
    flags = jnp.stack([low, band_index == sources - 1]).astype(jnp.int32)

    ya = jnp.arange(pairs, dtype=jnp.int32)
    p = jnp.arange(LANES, dtype=jnp.int32)
    first = real_parts(*turn(ya[:, None] * ya[None, :], pairs))
    f1 = stacked(first.transpose(0, 2, 1, 3).reshape(2 * pairs, 2 * pairs))
    tw1 = jnp.stack(turn(ya[:, None] * p[None, :], length))
    yb = jnp.where(low, 0, LANES // 2) + jnp.arange(LANES // 2, dtype=jnp.int32)
    second = real_parts(*turn(yb[:, None] * p[None, :], LANES))
    second = second.transpose(2, 0, 1, 3).reshape(LANES, 2 * LANES)
    hi, lo = split_table(second)
    h = grid_and_rows(flags, own, par, kernel, f1, tw1, jnp.concatenate([hi, lo], axis=0), hi, sources, length)
    h = lax.all_to_all(h, ("sub", "vert"), split_axis=0, concat_axis=0, tiled=True)

    order = jnp.arange(sources, dtype=jnp.int32)
    order = jnp.where(low, order, sources - 1 - order)
    d = (bands * order[None, :] + jnp.arange(bands, dtype=jnp.int32)[:, None]).reshape(-1)
    xa = jnp.arange(LANES, dtype=jnp.int32)
    table = real_parts(*turn(xa[:, None] * d[None, :], LANES))
    hi, lo = split_table(table.transpose(1, 3, 0, 2).reshape(2 * PATCH, 2 * LANES))
    r = jnp.arange(PATCH, dtype=jnp.int32)
    tw2 = jnp.stack(turn(r[:, None] * xa[None, :], length))
    cos, sin = turn(r[:, None] * r[None, :], PATCH)
    last = jnp.concatenate([cos, jnp.where(r[None, :] == 0, 1.0, -sin)], axis=1) * scale
    return columns_of(
        flags, h, jnp.concatenate([hi, hi], axis=0), lo, tw2, stacked(last), sources, spans, bands, length
    )


def solution(mesh):
    au, vert = mesh.shape["au"], mesh.shape["vert"]
    halves = Mesh(mesh.devices.reshape(2, au // 2, vert), ("half", "sub", "vert"))
    rows = ("half", "sub")
    in_specs = (P(rows, "vert", None, None), P(rows, "vert", None, None), P(rows, "vert"), P())
    return jax.shard_map(
        functools.partial(local, au=au, vert=vert),
        mesh=halves,
        in_specs=in_specs,
        out_specs=P((*rows, "vert"), None),
        check_vma=False,
    )
```

```python
import functools
import math

import jax
import jax.numpy as jnp
from jax import lax
from jax.experimental import pallas as pl
from jax.experimental.pallas import tpu as pltpu
from jax.sharding import Mesh, PartitionSpec as P

PATCH = 64
LANES = 128
SUB = 8

BF16 = jnp.bfloat16
F32 = jnp.float32


def split(x):
    hi = x.astype(BF16)
    lo = (x - hi.astype(F32)).astype(BF16)
    return hi, lo


def dot(lhs, rhs):
    return lax.dot_general(lhs, rhs, (((1,), (0,)), ((), ())), preferred_element_type=F32)


def dot_nt(lhs, rhs):
    return lax.dot_general(lhs, rhs, (((1,), (1,)), ((), ())), preferred_element_type=F32)


def turn(product, length):
    angle = (2.0 * math.pi / length) * (product % length).astype(F32)
    return jnp.cos(angle), jnp.sin(angle)


def real_parts(cos, sin):
    return jnp.stack([jnp.stack([cos, -sin]), jnp.stack([sin, cos])])


def tap_blocks(kern, cells, base, mirrored, length, wrap):
    slots = cells.shape[1]
    shape = (SUB, slots)
    cell = lax.shift_right_logical(cells, 7)
    fine = jnp.broadcast_to(cells & 127, shape)
    taps = jnp.take_along_axis(kern, fine, axis=1, mode="promise_in_bounds")
    sub = lax.broadcasted_iota(jnp.int32, shape, 0)
    taps = jnp.where(jnp.broadcast_to(cell, shape) + sub < length, taps, 0.0)
    off = jnp.broadcast_to(cell & (PATCH - 1), shape)
    if mirrored:
        place = base + PATCH - off
        tap = (place - sub) & (SUB - 1)
        block = lax.shift_right_arithmetic(place - tap, 3)
    else:
        place = base + off
        tap = (sub - place) & (SUB - 1)
        block = lax.shift_right_arithmetic(place + tap, 3)
    if wrap:
        block = block & (wrap - 1)
    turned = jnp.take_along_axis(taps, tap, axis=0, mode="promise_in_bounds")
    return turned, block


def patch_operands(kern, fields, mirrored, parity, length):
    values_re, values_im = fields[0:1], fields[1:2]
    cells = fields[2:4].astype(jnp.int32)
    rows, row_block = tap_blocks(kern, cells[0:1], SUB, mirrored, length, 0)
    cols, col_block = tap_blocks(kern, cells[1:2], PATCH * parity, mirrored, length, 2 * PATCH // SUB)
    if mirrored:
        values_im = -values_im

    def halves(x):
        hi = x.astype(BF16).astype(F32)
        return hi, x - hi

    row_masks = [row_block == j for j in range(PATCH // SUB + 2)]
    a_hi, a_lo = [], []
    for value in (values_re, values_im):
        hi, lo = halves(rows * value)
        a_hi += [jnp.where(m, hi, 0.0) for m in row_masks]
        a_lo += [jnp.where(m, lo, 0.0) for m in row_masks]
    col_hi, col_lo = halves(cols)
    col_masks = [col_block == j for j in range(2 * PATCH // SUB)]
    live = [(j - parity * (PATCH // SUB)) % len(col_masks) in (*range(9), 15) for j in range(len(col_masks))]
    zero = jnp.zeros_like(cols)
    b = [jnp.where(m, x, 0.0) if on else zero for x in (col_hi, col_lo) for m, on in zip(col_masks, live)]
    return jnp.concatenate(a_hi + a_lo, axis=0).astype(BF16), jnp.concatenate(b, axis=0).astype(BF16)


def tile_of(kern, low, high, parity, length):
    low_a, low_b = patch_operands(kern, low, False, parity, length)
    high_a, high_b = patch_operands(kern, high, True, parity, length)
    a = jnp.concatenate([low_a, high_a], axis=1)
    b = jnp.concatenate([low_b, high_b], axis=1)
    rows = a.shape[0] // 2
    out = dot_nt(a, b)
    return out[:rows, :LANES] + out[:rows, LANES:] + out[rows:, :LANES]


def grid_kernel(dims, *refs):
    pairs, row_stride, length, first_band, last_band = dims
    last_ref, low_ref, high_ref, kern_ref, f1_ref, tw_ref, eh_ref, el_ref = refs[:8]
    refs = refs[8:]
    if not first_band:
        in_ref, refs = refs[0], refs[1:]
    h_ref, refs = refs[0], refs[1:]
    if not last_band:
        out_ref, refs = refs[0], refs[1:]
    g_ref, carry_ref = refs
    spill = 2 * SUB
    tile_rows = PATCH + spill
    rows = tile_rows if last_band else PATCH
    is_last = last_ref[0] == 1
    kern = kern_ref[...]
    parts = 2 * pairs
    lane = lax.broadcasted_iota(jnp.int32, (2 * tile_rows, LANES), 1)

    def columns(q):
        nxt = jnp.where(q == pairs - 1, 0, q + 1)
        odd = tile_of(kern, low_ref[q, 4:8, :], high_ref[pairs - 1 - q, 0:4, :], 1, length)
        even = tile_of(kern, low_ref[nxt, 0:4, :], high_ref[pairs - 1 - nxt, 4:8, :], 0, length)
        here = jnp.where(lane < SUB, 0.0, odd) + jnp.where(lane < LANES - SUB, 0.0, even)
        there = jnp.where(lane < SUB, odd, 0.0) + jnp.where(lane < LANES - SUB, even, 0.0)
        return here, there

    _, there = columns(pairs - 1)
    carry_ref[...] = there

    def step(q, _):
        here, there = columns(q)
        total = here + carry_ref[...]
        carry_ref[...] = there
        for part in range(2):
            value = total[part * tile_rows : (part + 1) * tile_rows]
            at = part * pairs + q
            base = pl.multiple_of(at * row_stride, SUB)
            shared = pl.ds(pl.multiple_of(at * spill, SUB), spill)
            top = value[:spill]
            if not first_band:
                top = top + in_ref[shared, :]
            g_ref[pl.ds(base, spill), :] = top
            g_ref[pl.ds(base + spill, rows - spill), :] = value[spill:rows]
            if not last_band:
                out_ref[shared, :] = value[rows:]
        return 0

    lax.fori_loop(0, pairs, step, 0, unroll=GRID_UNROLL)

    cos = tw_ref[0]
    sin = tw_ref[1]

    def quad(group, _):
        lines = []
        for pair in range(2):
            cells = []
            for one in range(2):
                row = 4 * group + 2 * pair + one
                if last_band:
                    j = row - PATCH - SUB
                    moved = jnp.where(j == 6, 0, jnp.where(j == 7, 7, jnp.where(j % 2 == 0, j + 2, j)))
                    row = jnp.where(is_last & (j >= 0), PATCH + SUB + moved, row)
                cells.append(g_ref[pl.ds(row, parts, stride=row_stride), :])
            hi, lo = split(jnp.concatenate(cells, axis=1))
            out = dot(f1_ref[...], jnp.concatenate([hi, lo], axis=0))
            out = out[:parts] + out[parts:]
            for one in range(2):
                re = out[:pairs, one * LANES : (one + 1) * LANES]
                im = out[pairs:, one * LANES : (one + 1) * LANES]
                lines.append(jnp.concatenate([re * cos - im * sin, re * sin + im * cos], axis=1))
        hi, lo = split(jnp.concatenate(lines, axis=0))
        count = el_ref.shape[0]
        out = dot_nt(eh_ref[...], hi)
        out = out[:count] + out[count:] + dot_nt(el_ref[...], lo)
        dests, _, share, _ = h_ref.shape
        for part in range(2):
            piece = out[:, part * LANES : (part + 1) * LANES].reshape(dests, share, LANES)
            h_ref[:, 2 * group + part, :, :] = piece
        return 0

    lax.fori_loop(0, rows // 4, quad, 0, unroll=QUAD_UNROLL)


GRID_UNROLL = 8
QUAD_UNROLL = 8


def grid_and_rows(last, low, high, kern, tables, carry, dests, length, last_band):
    pairs = low.shape[0]
    spill = 2 * SUB
    rows = PATCH + spill if last_band else PATCH
    row_stride = rows + SUB
    outs = tables[3].shape[0]
    shared = (2 * pairs * spill, LANES)
    vmem = pl.BlockSpec(memory_space=pltpu.VMEM)
    out_shape = [jax.ShapeDtypeStruct((dests, rows * pairs // LANES, outs // dests, LANES), F32)]
    if not last_band:
        out_shape.append(jax.ShapeDtypeStruct(shared, F32))
    args = [low, high, kern, *tables] + ([] if carry is None else [carry])
    out = pl.pallas_call(
        functools.partial(grid_kernel, (pairs, row_stride, length, carry is None, last_band)),
        out_shape=out_shape,
        in_specs=[pl.BlockSpec(memory_space=pltpu.SMEM)] + [vmem] * len(args),
        out_specs=[vmem] * len(out_shape),
        scratch_shapes=[
            pltpu.VMEM((2 * pairs * row_stride, LANES), F32),
            pltpu.VMEM((2 * (PATCH + spill), LANES), F32),
        ],
        compiler_params=pltpu.CompilerParams(vmem_limit_bytes=40 * 1024 * 1024),
        cost_estimate=pl.CostEstimate(flops=20 * 10**9, bytes_accessed=8 * 2**20, transcendentals=0),
        name="grid_rows",
    )(last, *args)
    return out if not last_band else (out[0], None)


def column_kernel(dims, flags_ref, *refs):
    sources, spans, bands, block_rows = dims
    h_refs = refs[:bands]
    f2_ref, f2l_ref, tw_ref, e2_ref, out_ref, r_ref, z_ref, s_ref, sems = refs[bands:]
    share = 2 * spans
    low = flags_ref[0] == 1
    width = LANES
    y_count = spans * PATCH
    half = PATCH // 2

    blocks = sum(ref.shape[1] for ref in h_refs)
    stride = (blocks + 1) * share

    @pl.when(pl.program_id(0) == 0)
    def _():
        copies = [
            pltpu.make_async_copy(
                ref.at[n], r_ref.at[pl.ds(n * (blocks + 1) + i * half, ref.shape[1])], sems.at[i * sources + n]
            )
            for n in range(sources)
            for i, ref in enumerate(h_refs)
        ]
        for copy in copies:
            copy.start()
        for copy in copies:
            copy.wait()
        flat = r_ref.reshape(sources * stride, width)
        up_block = SUB // 2 + bands * half
        sub = lax.broadcasted_iota(jnp.int32, (share, width), 0)
        sign = jnp.where(sub % 2 == 0, 1.0, -1.0)

        def at_block(n, block):
            source = jnp.where(low, n, sources - 1 - n)
            return source * (blocks + 1) + block

        def add(to, value):
            r_ref[to] = r_ref[to] + value

        def neighbours(n, _):
            for t in range(SUB // 2):
                add(at_block(n + 1, SUB // 2 + t), r_ref[at_block(n, up_block + t)])
                add(at_block(n, up_block - SUB // 2 + t), r_ref[at_block(n + 1, t)])
            return 0

        lax.fori_loop(0, sources - 1, neighbours, 0)
        for t in range(SUB // 2 - 1):
            add(at_block(sources - 1, up_block - 1 - t), sign * r_ref[at_block(sources - 1, up_block + t)])
        top = r_ref[at_block(sources - 1, up_block + SUB // 2 - 1)]
        lane = lax.broadcasted_iota(jnp.int32, (share, width), 1)
        lifted = jnp.concatenate([top[share - 1 :], top[: share - 1]], axis=0)
        first = at_block(0, SUB // 2)
        r_ref[first] = jnp.where((sub % 2 == 1) & (lane < PATCH), lifted, r_ref[first])

        odd = lax.broadcasted_iota(jnp.int32, (PATCH, width), 1) % 2
        flip = jnp.where(odd == 0, 1.0, -1.0)

        def pair_step(rho, _):
            tall = []
            for k in range(spans):
                cells = []
                for c in range(2):
                    for i in range(bands):
                        row = (SUB // 2 + i * half + rho) * share + 2 * k + c
                        cells.append(flat[pl.ds(row, sources, stride=stride), :])
                tall.append(jnp.concatenate(cells, axis=0).T)
            x = jnp.concatenate(tall, axis=0)
            hi, lo = split(x)
            z = dot(jnp.concatenate([hi, lo], axis=1), f2_ref[...]) + dot(hi, f2l_ref[...])
            top_col = jnp.where(low, x[:, PATCH : PATCH + 1], x[:, PATCH + sources - 1 : PATCH + sources])
            for k in range(spans):
                for one in range(2):
                    at = (2 * k + one) * PATCH
                    re = z[at : at + PATCH, :width]
                    im = z[at : at + PATCH, width:]
                    line = 2 * rho + one
                    cos = tw_ref[0, pl.ds(line, 1), :]
                    sin = tw_ref[1, pl.ds(line, 1), :]
                    new_re = re * cos - im * sin
                    new_im = re * sin + im * cos
                    if one == 0:
                        nyquist = flip * top_col[at : at + PATCH]
                        new_im = jnp.where(rho == 0, nyquist, new_im)
                    z_ref[pl.ds(pl.multiple_of(line * y_count + k * PATCH, PATCH), PATCH), :] = new_re
                    z_ref[pl.ds(pl.multiple_of((PATCH + line) * y_count + k * PATCH, PATCH), PATCH), :] = new_im
            return 0

        lax.fori_loop(0, half, pair_step, 0)

    start = pl.program_id(0) * block_rows

    def eight(group, _):
        for pair in range(SUB // 2):
            y = start + group * SUB + 2 * pair
            cells = [z_ref[pl.ds(y + one, 2 * PATCH, stride=y_count), :] for one in range(2)]
            hi, lo = split(jnp.concatenate(cells, axis=1))
            out = dot(e2_ref[...], jnp.concatenate([hi, lo], axis=0))
            out = out[:PATCH] + out[PATCH:]
            for one in range(2):
                s_ref[pl.ds(2 * pair + one, PATCH, stride=SUB), :] = out[:, one * width : (one + 1) * width]
        at = pl.ds(pl.multiple_of(group * SUB, SUB), SUB)
        for block in range(PATCH):
            out_ref[at, block * width : (block + 1) * width] = s_ref[block * SUB : (block + 1) * SUB, :]
        return 0

    lax.fori_loop(0, block_rows // SUB, eight, 0)


def columns_of(flags, hs, f2, f2l, tw, e2, sources, spans, bands, length):
    y_count = spans * PATCH
    block_rows = min(32, y_count)
    vmem = pl.BlockSpec(memory_space=pltpu.VMEM)
    return pl.pallas_call(
        functools.partial(column_kernel, (sources, spans, bands, block_rows)),
        grid=(y_count // block_rows,),
        out_shape=jax.ShapeDtypeStruct((y_count, length), F32),
        in_specs=[pl.BlockSpec(memory_space=pltpu.SMEM)] + [pl.BlockSpec(memory_space=pl.ANY)] * bands + [vmem] * 4,
        out_specs=pl.BlockSpec((block_rows, length), lambda n: (n, 0)),
        scratch_shapes=[
            pltpu.VMEM((sources * (sum(h.shape[1] for h in hs) + 1), hs[0].shape[2], LANES), F32),
            pltpu.VMEM((2 * PATCH * y_count, LANES), F32),
            pltpu.VMEM((PATCH * SUB, LANES), F32),
            pltpu.SemaphoreType.DMA((sources * bands,)),
        ],
        compiler_params=pltpu.CompilerParams(vmem_limit_bytes=60 * 1024 * 1024),
        name="columns",
    )(flags, *hs, f2, f2l, tw, e2)


def split_table(x):
    rounded = lax.reduce_precision(x, 8, 7)
    return rounded.astype(BF16), (x - rounded).astype(BF16)


def stacked(table):
    hi, lo = split_table(table)
    return jnp.concatenate([jnp.concatenate([hi, hi], axis=1), jnp.concatenate([lo, jnp.zeros_like(lo)], axis=1)], axis=0)


def local(vis_value, vis_pos, counts, kernel, *, au, vert):
    devices = au * vert
    axes = ("half", "sub", "vert")
    me = lax.axis_index(axes)
    low = me < devices // 2
    slots = vis_value.shape[3]
    bands = vis_value.shape[0] // vert
    local_cols = vis_value.shape[1]
    cols = local_cols * vert
    pairs = cols // 2
    length = cols * PATCH
    rows_of_patches = vis_value.shape[0] * au
    scale = 1.0 / math.sqrt(rows_of_patches * cols * slots)
    sources = devices // 2
    y_count = length // devices
    spans = y_count // PATCH

    live = jnp.arange(slots, dtype=jnp.int32) < counts[:, :, None, None]
    fields = jnp.concatenate([jnp.where(live, vis_value, 0.0), vis_pos.astype(F32)], axis=2)
    fields = fields.reshape(vert, bands, local_cols // 2, 8, slots)
    own = lax.all_to_all(fields, "vert", split_axis=0, concat_axis=2, tiled=True)
    own = own.reshape(bands, pairs, 8, slots)
    mirror = [(d, devices - 1 - d) for d in range(devices)]
    sent = jnp.where(low, own, own[::-1])
    received = [lax.ppermute(sent[:1], axes, mirror)]
    if bands > 1:
        received.append(lax.ppermute(sent[1:], axes, mirror))

    band_index = jnp.where(low, me, devices - 1 - me)
    flags = low.astype(jnp.int32)[None]
    last = (band_index == sources - 1).astype(jnp.int32)[None]

    ya = jnp.arange(pairs, dtype=jnp.int32)
    p = jnp.arange(LANES, dtype=jnp.int32)
    first = real_parts(*turn(ya[:, None] * ya[None, :], pairs))
    f1 = stacked(first.transpose(0, 2, 1, 3).reshape(2 * pairs, 2 * pairs))
    tw1 = jnp.stack(turn(ya[:, None] * p[None, :], length))
    yb = jnp.where(low, 0, LANES // 2) + jnp.arange(LANES // 2, dtype=jnp.int32)
    second = real_parts(*turn(yb[:, None] * p[None, :], LANES))
    second = second.transpose(2, 0, 1, 3).reshape(LANES, 2 * LANES)
    hi, lo = split_table(second)
    tables = (f1, tw1, jnp.concatenate([hi, lo], axis=0), hi)
    carry, hs = None, []
    for band in range(bands):
        got = received[0][0] if band == 0 else received[1][band - 1]
        low_patches = jnp.where(low, own[band], got)
        high_patches = jnp.where(low, got, own[bands - 1 - band])
        h, carry = grid_and_rows(
            last, low_patches, high_patches, kernel, tables, carry, sources, length, band == bands - 1
        )
        hs.append(lax.all_to_all(h, ("sub", "vert"), split_axis=0, concat_axis=0, tiled=True))

    order = jnp.arange(sources, dtype=jnp.int32)
    order = jnp.where(low, order, sources - 1 - order)
    d = (bands * order[None, :] + jnp.arange(bands, dtype=jnp.int32)[:, None]).reshape(-1)
    xa = jnp.arange(LANES, dtype=jnp.int32)
    table = real_parts(*turn(xa[:, None] * d[None, :], LANES))
    hi, lo = split_table(table.transpose(1, 3, 0, 2).reshape(2 * PATCH, 2 * LANES))
    r = jnp.arange(PATCH, dtype=jnp.int32)
    tw2 = jnp.stack(turn(r[:, None] * xa[None, :], length))
    cos, sin = turn(r[:, None] * r[None, :], PATCH)
    last = jnp.concatenate([cos, jnp.where(r[None, :] == 0, 1.0, -sin)], axis=1) * scale
    return columns_of(
        flags, hs, jnp.concatenate([hi, hi], axis=0), lo, tw2, stacked(last), sources, spans, bands, length
    )


def solution(mesh):
    au, vert = mesh.shape["au"], mesh.shape["vert"]
    halves = Mesh(mesh.devices.reshape(2, au // 2, vert), ("half", "sub", "vert"))
    rows = ("half", "sub")
    in_specs = (P(rows, "vert", None, None), P(rows, "vert", None, None), P(rows, "vert"), P())

    def program(*args):
        return local(*args, au=au, vert=vert)

    return jax.shard_map(
        program,
        mesh=halves,
        in_specs=in_specs,
        out_specs=P((*rows, "vert"), None),
        check_vma=False,
    )
```

```python
import functools
import math

import jax
import jax.numpy as jnp
from jax import lax
from jax.experimental import pallas as pl
from jax.experimental.pallas import tpu as pltpu
from jax.sharding import Mesh, PartitionSpec as P

PATCH = 64
LANES = 128
SUB = 8

BF16 = jnp.bfloat16
F32 = jnp.float32


def split(x):
    hi = x.astype(BF16)
    lo = (x - hi.astype(F32)).astype(BF16)
    return hi, lo


def dot(lhs, rhs):
    return lax.dot_general(lhs, rhs, (((1,), (0,)), ((), ())), preferred_element_type=F32)


def dot_nt(lhs, rhs):
    return lax.dot_general(lhs, rhs, (((1,), (1,)), ((), ())), preferred_element_type=F32)


def turn(product, length):
    angle = (2.0 * math.pi / length) * (product % length).astype(F32)
    return jnp.cos(angle), jnp.sin(angle)


def real_parts(cos, sin):
    return jnp.stack([jnp.stack([cos, -sin]), jnp.stack([sin, cos])])


def tap_blocks(kern, cells, base, mirrored, length, wrap):
    slots = cells.shape[1]
    shape = (SUB, slots)
    cell = lax.shift_right_logical(cells, 7)
    fine = jnp.broadcast_to(cells & 127, shape)
    taps = jnp.take_along_axis(kern, fine, axis=1, mode="promise_in_bounds")
    sub = lax.broadcasted_iota(jnp.int32, shape, 0)
    taps = jnp.where(jnp.broadcast_to(cell, shape) + sub < length, taps, 0.0)
    off = jnp.broadcast_to(cell & (PATCH - 1), shape)
    if mirrored:
        place = base + PATCH - off
        tap = (place - sub) & (SUB - 1)
        block = lax.shift_right_arithmetic(place - tap, 3)
    else:
        place = base + off
        tap = (sub - place) & (SUB - 1)
        block = lax.shift_right_arithmetic(place + tap, 3)
    if wrap:
        block = block & (wrap - 1)
    turned = jnp.take_along_axis(taps, tap, axis=0, mode="promise_in_bounds")
    return turned, block


def patch_operands(kern, fields, mirrored, parity, length):
    values_re, values_im = fields[0:1], fields[1:2]
    cells = fields[2:4].astype(jnp.int32)
    rows, row_block = tap_blocks(kern, cells[0:1], SUB, mirrored, length, 0)
    cols, col_block = tap_blocks(kern, cells[1:2], PATCH * parity, mirrored, length, 2 * PATCH // SUB)
    if mirrored:
        values_im = -values_im

    def halves(x):
        hi = x.astype(BF16).astype(F32)
        return hi, x - hi

    row_masks = [row_block == j for j in range(PATCH // SUB + 2)]
    a_hi, a_lo = [], []
    for value in (values_re, values_im):
        hi, lo = halves(rows * value)
        a_hi += [jnp.where(m, hi, 0.0) for m in row_masks]
        a_lo += [jnp.where(m, lo, 0.0) for m in row_masks]
    col_hi, col_lo = halves(cols)
    col_masks = [col_block == j for j in range(2 * PATCH // SUB)]
    live = [(j - parity * (PATCH // SUB)) % len(col_masks) in (*range(9), 15) for j in range(len(col_masks))]
    zero = jnp.zeros_like(cols)
    b = [jnp.where(m, x, 0.0) if on else zero for x in (col_hi, col_lo) for m, on in zip(col_masks, live)]
    return jnp.concatenate(a_hi + a_lo, axis=0).astype(BF16), jnp.concatenate(b, axis=0).astype(BF16)


def tile_of(kern, low, high, parity, length):
    low_a, low_b = patch_operands(kern, low, False, parity, length)
    high_a, high_b = patch_operands(kern, high, True, parity, length)
    a = jnp.concatenate([low_a, high_a], axis=1)
    b = jnp.concatenate([low_b, high_b], axis=1)
    rows = a.shape[0] // 2
    out = dot_nt(a, b)
    return out[:rows, :LANES] + out[:rows, LANES:] + out[rows:, :LANES]


def grid_kernel(dims, *refs):
    pairs, row_stride, length, first_band, last_band = dims
    last_ref, low_ref, high_ref, kern_ref, f1_ref, tw_ref, eh_ref, el_ref = refs[:8]
    refs = refs[8:]
    if not first_band:
        in_ref, refs = refs[0], refs[1:]
    h_ref, refs = refs[0], refs[1:]
    if not last_band:
        out_ref, refs = refs[0], refs[1:]
    g_ref, carry_ref = refs
    spill = 2 * SUB
    tile_rows = PATCH + spill
    rows = tile_rows if last_band else PATCH
    is_last = last_ref[0] == 1
    kern = kern_ref[...]
    parts = 2 * pairs
    lane = lax.broadcasted_iota(jnp.int32, (2 * tile_rows, LANES), 1)

    def columns(q):
        nxt = jnp.where(q == pairs - 1, 0, q + 1)
        odd = tile_of(kern, low_ref[q, 4:8, :], high_ref[pairs - 1 - q, 0:4, :], 1, length)
        even = tile_of(kern, low_ref[nxt, 0:4, :], high_ref[pairs - 1 - nxt, 4:8, :], 0, length)
        here = jnp.where(lane < SUB, 0.0, odd) + jnp.where(lane < LANES - SUB, 0.0, even)
        there = jnp.where(lane < SUB, odd, 0.0) + jnp.where(lane < LANES - SUB, even, 0.0)
        return here, there

    _, there = columns(pairs - 1)
    carry_ref[...] = there

    def step(q, _):
        here, there = columns(q)
        total = here + carry_ref[...]
        carry_ref[...] = there
        for part in range(2):
            value = total[part * tile_rows : (part + 1) * tile_rows]
            at = part * pairs + q
            base = pl.multiple_of(at * row_stride, SUB)
            shared = pl.ds(pl.multiple_of(at * spill, SUB), spill)
            top = value[:spill]
            if not first_band:
                top = top + in_ref[shared, :]
            g_ref[pl.ds(base, spill), :] = top
            g_ref[pl.ds(base + spill, rows - spill), :] = value[spill:rows]
            if not last_band:
                out_ref[shared, :] = value[rows:]
        return 0

    lax.fori_loop(0, pairs, step, 0, unroll=GRID_UNROLL)

    cos = tw_ref[0]
    sin = tw_ref[1]

    def quad(group, _):
        lines = []
        for pair in range(2):
            cells = []
            for one in range(2):
                row = 4 * group + 2 * pair + one
                if last_band:
                    j = row - PATCH - SUB
                    moved = jnp.where(j == 6, 0, jnp.where(j == 7, 7, jnp.where(j % 2 == 0, j + 2, j)))
                    row = jnp.where(is_last & (j >= 0), PATCH + SUB + moved, row)
                cells.append(g_ref[pl.ds(row, parts, stride=row_stride), :])
            hi, lo = split(jnp.concatenate(cells, axis=1))
            out = dot(f1_ref[...], jnp.concatenate([hi, lo], axis=0))
            out = out[:parts] + out[parts:]
            for one in range(2):
                re = out[:pairs, one * LANES : (one + 1) * LANES]
                im = out[pairs:, one * LANES : (one + 1) * LANES]
                lines.append(jnp.concatenate([re * cos - im * sin, re * sin + im * cos], axis=1))
        hi, lo = split(jnp.concatenate(lines, axis=0))
        count = el_ref.shape[0]
        out = dot_nt(eh_ref[...], hi)
        out = out[:count] + out[count:] + dot_nt(el_ref[...], lo)
        dests, _, share, _ = h_ref.shape
        for part in range(2):
            piece = out[:, part * LANES : (part + 1) * LANES].reshape(dests, share, LANES)
            h_ref[:, 2 * group + part, :, :] = piece
        return 0

    lax.fori_loop(0, rows // 4, quad, 0, unroll=QUAD_UNROLL)


GRID_UNROLL = 8
QUAD_UNROLL = 8


def grid_and_rows(last, low, high, kern, tables, carry, dests, length, last_band):
    pairs = low.shape[0]
    spill = 2 * SUB
    rows = PATCH + spill if last_band else PATCH
    row_stride = rows + SUB
    outs = tables[3].shape[0]
    shared = (2 * pairs * spill, LANES)
    vmem = pl.BlockSpec(memory_space=pltpu.VMEM)
    out_shape = [jax.ShapeDtypeStruct((dests, rows * pairs // LANES, outs // dests, LANES), F32)]
    if not last_band:
        out_shape.append(jax.ShapeDtypeStruct(shared, F32))
    args = [low, high, kern, *tables] + ([] if carry is None else [carry])
    out = pl.pallas_call(
        functools.partial(grid_kernel, (pairs, row_stride, length, carry is None, last_band)),
        out_shape=out_shape,
        in_specs=[pl.BlockSpec(memory_space=pltpu.SMEM)] + [vmem] * len(args),
        out_specs=[vmem] * len(out_shape),
        scratch_shapes=[
            pltpu.VMEM((2 * pairs * row_stride, LANES), F32),
            pltpu.VMEM((2 * (PATCH + spill), LANES), F32),
        ],
        compiler_params=pltpu.CompilerParams(vmem_limit_bytes=40 * 1024 * 1024),
        cost_estimate=pl.CostEstimate(flops=20 * 10**9, bytes_accessed=8 * 2**20, transcendentals=0),
        name="grid_rows",
    )(last, *args)
    return out if not last_band else (out[0], None)


def column_kernel(dims, flags_ref, *refs):
    sources, spans, bands, block_rows, vert = dims
    h_refs = refs[:bands]
    f2_ref, f2l_ref, tw_ref, e2_ref, out_ref, r_ref, z_ref, s_ref = refs[bands:]
    share = 2 * spans
    low = flags_ref[0] == 1
    width = LANES
    z_pitch = spans * PATCH + SUB
    half = PATCH // 2

    blocks = sum(ref.shape[1] for ref in h_refs)
    stride = (blocks + 1) * share

    @pl.when(pl.program_id(0) == 0)
    def _():
        def arrived(n, _):
            for i, ref in enumerate(h_refs):
                r_ref[pl.ds(n * (blocks + 1) + i * half, ref.shape[1])] = ref[n]
            return 0

        lax.fori_loop(0, sources, arrived, 0)
        flat = r_ref.reshape(sources * stride, width)
        up_block = SUB // 2 + bands * half
        sub = lax.broadcasted_iota(jnp.int32, (share, width), 0)
        sign = jnp.where(sub % 2 == 0, 1.0, -1.0)

        def at_block(n, block):
            source = jnp.where(low, n, backwards(n, vert, sources // vert))
            return source * (blocks + 1) + block

        def add(to, value):
            r_ref[to] = r_ref[to] + value

        def neighbours(n, _):
            for t in range(SUB // 2):
                add(at_block(n + 1, SUB // 2 + t), r_ref[at_block(n, up_block + t)])
                add(at_block(n, up_block - SUB // 2 + t), r_ref[at_block(n + 1, t)])
            return 0

        lax.fori_loop(0, sources - 1, neighbours, 0)
        for t in range(SUB // 2 - 1):
            add(at_block(sources - 1, up_block - 1 - t), sign * r_ref[at_block(sources - 1, up_block + t)])
        top = r_ref[at_block(sources - 1, up_block + SUB // 2 - 1)]
        lane = lax.broadcasted_iota(jnp.int32, (share, width), 1)
        lifted = jnp.concatenate([top[share - 1 :], top[: share - 1]], axis=0)
        first = at_block(0, SUB // 2)
        r_ref[first] = jnp.where((sub % 2 == 1) & (lane < PATCH), lifted, r_ref[first])

        odd = lax.broadcasted_iota(jnp.int32, (PATCH, width), 1) % 2
        flip = jnp.where(odd == 0, 1.0, -1.0)

        def pair_step(rho, _):
            tall = []
            for k in range(spans):
                cells = []
                for c in range(2):
                    for i in range(bands):
                        row = (SUB // 2 + i * half + rho) * share + 2 * k + c
                        cells.append(flat[pl.ds(row, sources, stride=stride), :])
                tall.append(jnp.concatenate(cells, axis=0).T)
            x = jnp.concatenate(tall, axis=0)
            hi, lo = split(x)
            z = dot(jnp.concatenate([hi, lo], axis=1), f2_ref[...]) + dot(hi, f2l_ref[...])
            top_col = jnp.where(low, x[:, PATCH : PATCH + 1], x[:, PATCH + sources - vert : PATCH + sources - vert + 1])
            for k in range(spans):
                for one in range(2):
                    at = (2 * k + one) * PATCH
                    re = z[at : at + PATCH, :width]
                    im = z[at : at + PATCH, width:]
                    line = 2 * rho + one
                    cos = tw_ref[0, pl.ds(line, 1), :]
                    sin = tw_ref[1, pl.ds(line, 1), :]
                    new_re = re * cos - im * sin
                    new_im = re * sin + im * cos
                    if one == 0:
                        nyquist = flip * top_col[at : at + PATCH]
                        new_im = jnp.where(rho == 0, nyquist, new_im)
                    z_ref[pl.ds(pl.multiple_of(line * z_pitch + k * PATCH, SUB), PATCH), :] = new_re
                    z_ref[pl.ds(pl.multiple_of((PATCH + line) * z_pitch + k * PATCH, SUB), PATCH), :] = new_im
            return 0

        lax.fori_loop(0, half, pair_step, 0, unroll=4)

    start = pl.program_id(0) * block_rows

    def eight(group, _):
        for pair in range(SUB // 2):
            y = start + group * SUB + 2 * pair
            cells = [z_ref[pl.ds(y + one, 2 * PATCH, stride=z_pitch), :] for one in range(2)]
            hi, lo = split(jnp.concatenate(cells, axis=1))
            out = dot(e2_ref[...], jnp.concatenate([hi, lo], axis=0))
            out = out[:PATCH] + out[PATCH:]
            for one in range(2):
                s_ref[pl.ds(2 * pair + one, PATCH, stride=SUB), :] = out[:, one * width : (one + 1) * width]
        at = pl.ds(pl.multiple_of(group * SUB, SUB), SUB)
        for block in range(PATCH):
            out_ref[at, block * width : (block + 1) * width] = s_ref[block * SUB : (block + 1) * SUB, :]
        return 0

    lax.fori_loop(0, block_rows // SUB, eight, 0, unroll=4)


def columns_of(flags, hs, f2, f2l, tw, e2, sources, spans, bands, vert, length):
    y_count = spans * PATCH
    block_rows = min(32, y_count)
    vmem = pl.BlockSpec(memory_space=pltpu.VMEM)
    return pl.pallas_call(
        functools.partial(column_kernel, (sources, spans, bands, block_rows, vert)),
        grid=(y_count // block_rows,),
        out_shape=jax.ShapeDtypeStruct((y_count, length), F32),
        in_specs=[pl.BlockSpec(memory_space=pltpu.SMEM)] + [vmem] * (bands + 4),
        out_specs=pl.BlockSpec((block_rows, length), lambda n: (n, 0)),
        scratch_shapes=[
            pltpu.VMEM((sources * (sum(h.shape[1] for h in hs) + 1), hs[0].shape[2], LANES), F32),
            pltpu.VMEM((2 * PATCH * (y_count + SUB), LANES), F32),
            pltpu.VMEM((PATCH * SUB, LANES), F32),
        ],
        compiler_params=pltpu.CompilerParams(vmem_limit_bytes=60 * 1024 * 1024),
        name="columns",
    )(flags, *hs, f2, f2l, tw, e2)


def split_table(x):
    rounded = lax.reduce_precision(x, 8, 7)
    return rounded.astype(BF16), (x - rounded).astype(BF16)


def stacked(table):
    hi, lo = split_table(table)
    return jnp.concatenate([jnp.concatenate([hi, hi], axis=1), jnp.concatenate([lo, jnp.zeros_like(lo)], axis=1)], axis=0)


def backwards(n, vert, count):
    return (count - 1 - n // vert) * vert + n % vert


def local(vis_value, vis_pos, counts, kernel, *, au, vert):
    devices = au * vert
    half_au = au // 2
    axes = ("half", "sub", "vert")
    me = lax.axis_index(axes)
    low = me < devices // 2
    slots = vis_value.shape[3]
    bands = vis_value.shape[0] // vert
    local_cols = vis_value.shape[1]
    cols = local_cols * vert
    pairs = cols // 2
    length = cols * PATCH
    rows_of_patches = vis_value.shape[0] * au
    scale = 1.0 / math.sqrt(rows_of_patches * cols * slots)
    sources = devices // 2
    y_count = length // devices
    spans = y_count // PATCH

    live = jnp.arange(slots, dtype=jnp.int32) < counts[:, :, None, None]
    fields = jnp.concatenate([jnp.where(live, vis_value, 0.0), vis_pos.astype(F32)], axis=2)
    fields = fields.reshape(vert, bands, local_cols // 2, 8, slots)
    fields = jnp.where(low, fields, fields[::-1])
    own = lax.all_to_all(fields, "vert", split_axis=0, concat_axis=2, tiled=True)
    own = own.reshape(bands, pairs, 8, slots)
    mirror = [(a * vert + v, (au - 1 - a) * vert + v) for a in range(au) for v in range(vert)]
    sent = jnp.where(low, own, own[::-1])
    received = [lax.ppermute(sent[:1], axes, mirror)]
    if bands > 1:
        later, first_piece = lax.optimization_barrier((sent[1:], received[0]))
        received = [first_piece, lax.ppermute(later, axes, mirror)]

    band_index = jnp.where(low, me, lax.axis_index("vert") + vert * (au - 1 - me // vert))
    flags = low.astype(jnp.int32)[None]
    last = (band_index == sources - 1).astype(jnp.int32)[None]

    ya = jnp.arange(pairs, dtype=jnp.int32)
    p = jnp.arange(LANES, dtype=jnp.int32)
    first = real_parts(*turn(ya[:, None] * ya[None, :], pairs))
    f1 = stacked(first.transpose(0, 2, 1, 3).reshape(2 * pairs, 2 * pairs))
    tw1 = jnp.stack(turn(ya[:, None] * p[None, :], length))
    yb = jnp.where(low, 0, LANES // 2) + jnp.arange(LANES // 2, dtype=jnp.int32)
    second = real_parts(*turn(yb[:, None] * p[None, :], LANES))
    second = second.transpose(2, 0, 1, 3).reshape(LANES, 2 * LANES)
    hi, lo = split_table(second)
    tables = (f1, tw1, jnp.concatenate([hi, lo], axis=0), hi)
    carry, hs = None, []
    for band in range(bands):
        got = received[0][0] if band == 0 else received[1][band - 1]
        low_patches = jnp.where(low, own[band], got)
        high_patches = jnp.where(low, got, own[bands - 1 - band])
        h, carry = grid_and_rows(
            last, low_patches, high_patches, kernel, tables, carry, sources, length, band == bands - 1
        )
        hs.append(lax.all_to_all(h, ("sub", "vert"), split_axis=0, concat_axis=0, tiled=True))

    order = jnp.arange(sources, dtype=jnp.int32)
    order = jnp.where(low, order, backwards(order, vert, half_au))
    d = (bands * order[None, :] + jnp.arange(bands, dtype=jnp.int32)[:, None]).reshape(-1)
    xa = jnp.arange(LANES, dtype=jnp.int32)
    table = real_parts(*turn(xa[:, None] * d[None, :], LANES))
    hi, lo = split_table(table.transpose(1, 3, 0, 2).reshape(2 * PATCH, 2 * LANES))
    r = jnp.arange(PATCH, dtype=jnp.int32)
    tw2 = jnp.stack(turn(r[:, None] * xa[None, :], length))
    cos, sin = turn(r[:, None] * r[None, :], PATCH)
    last = jnp.concatenate([cos, jnp.where(r[None, :] == 0, 1.0, -sin)], axis=1) * scale
    return columns_of(
        flags, hs, jnp.concatenate([hi, hi], axis=0), lo, tw2, stacked(last), sources, spans, bands, vert, length
    )


def solution(mesh):
    au, vert = mesh.shape["au"], mesh.shape["vert"]
    halves = Mesh(mesh.devices.reshape(2, au // 2, vert), ("half", "sub", "vert"))
    rows = ("half", "sub")
    in_specs = (P(rows, "vert", None, None), P(rows, "vert", None, None), P(rows, "vert"), P())

    def program(*args):
        return local(*args, au=au, vert=vert)

    return jax.shard_map(
        program,
        mesh=halves,
        in_specs=in_specs,
        out_specs=P((*rows, "vert"), None),
        check_vma=False,
    )
```

```python
import functools
import math

import jax
import jax.numpy as jnp
from jax import lax
from jax.experimental import pallas as pl
from jax.experimental.pallas import tpu as pltpu
from jax.sharding import Mesh, PartitionSpec as P

PATCH = 64
LANES = 128
SUB = 8

BF16 = jnp.bfloat16
F32 = jnp.float32
MESH = pl.DeviceIdType.MESH


def split(x):
    hi = x.astype(BF16)
    lo = (x - hi.astype(F32)).astype(BF16)
    return hi, lo


def dot(lhs, rhs):
    return lax.dot_general(lhs, rhs, (((1,), (0,)), ((), ())), preferred_element_type=F32)


def dot_nt(lhs, rhs):
    return lax.dot_general(lhs, rhs, (((1,), (1,)), ((), ())), preferred_element_type=F32)


def turn(product, length):
    angle = (2.0 * math.pi / length) * (product % length).astype(F32)
    return jnp.cos(angle), jnp.sin(angle)


def real_parts(cos, sin):
    return jnp.stack([jnp.stack([cos, -sin]), jnp.stack([sin, cos])])


def deal_kernel(dims, fields_ref, own_ref, got_ref, deal_sent, deal_came, mirror_sent, mirror_came, local_sem):
    halves, subs, vert = dims
    half, sub, v = (lax.axis_index(name) for name in ("half", "sub", "vert"))
    cols = fields_ref.shape[2]
    columns = pl.ds(v * cols, cols)
    mirror = (halves - 1 - half, subs - 1 - sub)
    there = [lax.rem(v + k, vert) for k in range(vert)]

    barrier = pltpu.get_barrier_semaphore()
    for k in range(vert):
        if k > 0:
            pl.semaphore_signal(barrier, inc=1, device_id=(half, sub, there[k]), device_id_type=MESH)
        pl.semaphore_signal(barrier, inc=1, device_id=(*mirror, there[k]), device_id_type=MESH)
    pl.semaphore_wait(barrier, 2 * vert - 1)

    copies = [
        pltpu.make_async_remote_copy(
            src_ref=fields_ref.at[there[k], 0],
            dst_ref=got_ref.at[columns],
            send_sem=mirror_sent.at[k],
            recv_sem=mirror_came.at[k],
            device_id=(*mirror, there[k]),
            device_id_type=MESH,
        )
        for k in range(vert)
    ] + [
        pltpu.make_async_remote_copy(
            src_ref=fields_ref.at[there[k]],
            dst_ref=own_ref.at[:, columns],
            send_sem=deal_sent.at[k],
            recv_sem=deal_came.at[k],
            device_id=(half, sub, there[k]),
            device_id_type=MESH,
        )
        for k in range(1, vert)
    ]
    copies.append(pltpu.make_async_copy(fields_ref.at[v], own_ref.at[:, columns], local_sem))
    for copy in copies:
        copy.start()
    for copy in copies:
        copy.wait()


def deal(fields, halves, subs):
    vert, bands, cols, lead, slots = fields.shape
    sems = pltpu.SemaphoreType.DMA((vert,))
    anywhere = pl.BlockSpec(memory_space=pl.ANY)
    return pl.pallas_call(
        functools.partial(deal_kernel, (halves, subs, vert)),
        out_shape=[
            jax.ShapeDtypeStruct((bands, vert * cols, lead, slots), fields.dtype),
            jax.ShapeDtypeStruct((vert * cols, lead, slots), fields.dtype),
        ],
        in_specs=[pl.BlockSpec(memory_space=pltpu.VMEM)],
        out_specs=[anywhere, anywhere],
        scratch_shapes=[sems, sems, sems, sems, pltpu.SemaphoreType.DMA],
        compiler_params=pltpu.CompilerParams(collective_id=0, has_side_effects=True),
        name="deal",
    )(fields)


def tap_blocks(kern, cells, base, mirrored, length, wrap):
    slots = cells.shape[1]
    shape = (SUB, slots)
    cell = lax.shift_right_logical(cells, 7)
    fine = jnp.broadcast_to(cells & 127, shape)
    taps = jnp.take_along_axis(kern, fine, axis=1, mode="promise_in_bounds")
    sub = lax.broadcasted_iota(jnp.int32, shape, 0)
    taps = jnp.where(jnp.broadcast_to(cell, shape) + sub < length, taps, 0.0)
    off = jnp.broadcast_to(cell & (PATCH - 1), shape)
    if mirrored:
        place = base + PATCH - off
        tap = (place - sub) & (SUB - 1)
        block = lax.shift_right_arithmetic(place - tap, 3)
    else:
        place = base + off
        tap = (sub - place) & (SUB - 1)
        block = lax.shift_right_arithmetic(place + tap, 3)
    if wrap:
        block = block & (wrap - 1)
    turned = jnp.take_along_axis(taps, tap, axis=0, mode="promise_in_bounds")
    return turned, block


def patch_operands(kern, fields, mirrored, parity, length):
    values_re, values_im = fields[0:1], fields[1:2]
    cells = fields[2:4].astype(jnp.int32)
    rows, row_block = tap_blocks(kern, cells[0:1], SUB, mirrored, length, 0)
    cols, col_block = tap_blocks(kern, cells[1:2], PATCH * parity, mirrored, length, 2 * PATCH // SUB)
    if mirrored:
        values_im = -values_im

    def halves(x):
        hi = x.astype(BF16).astype(F32)
        return hi, x - hi

    row_masks = [row_block == j for j in range(PATCH // SUB + 2)]
    a_hi, a_lo = [], []
    for value in (values_re, values_im):
        hi, lo = halves(rows * value)
        a_hi += [jnp.where(m, hi, 0.0) for m in row_masks]
        a_lo += [jnp.where(m, lo, 0.0) for m in row_masks]
    col_hi, col_lo = halves(cols)
    col_masks = [col_block == j for j in range(2 * PATCH // SUB)]
    live = [(j - parity * (PATCH // SUB)) % len(col_masks) in (*range(9), 15) for j in range(len(col_masks))]
    zero = jnp.zeros_like(cols)
    b = [jnp.where(m, x, 0.0) if on else zero for x in (col_hi, col_lo) for m, on in zip(col_masks, live)]
    return jnp.concatenate(a_hi + a_lo, axis=0).astype(BF16), jnp.concatenate(b, axis=0).astype(BF16)


def tile_of(kern, low, high, parity, length):
    low_a, low_b = patch_operands(kern, low, False, parity, length)
    high_a, high_b = patch_operands(kern, high, True, parity, length)
    a = jnp.concatenate([low_a, high_a], axis=1)
    b = jnp.concatenate([low_b, high_b], axis=1)
    rows = a.shape[0] // 2
    out = dot_nt(a, b)
    return out[:rows, :LANES] + out[:rows, LANES:] + out[rows:, :LANES]


def grid_kernel(dims, *refs):
    pairs, row_stride, length, first_band, last_band = dims
    last_ref, low_ref, high_ref, kern_ref, f1_ref, tw_ref, eh_ref, el_ref = refs[:8]
    refs = refs[8:]
    if not first_band:
        in_ref, refs = refs[0], refs[1:]
    h_ref, refs = refs[0], refs[1:]
    if not last_band:
        out_ref, refs = refs[0], refs[1:]
    g_ref, carry_ref = refs
    spill = 2 * SUB
    tile_rows = PATCH + spill
    rows = tile_rows if last_band else PATCH
    is_last = last_ref[0] == 1
    kern = kern_ref[...]
    parts = 2 * pairs
    lane = lax.broadcasted_iota(jnp.int32, (2 * tile_rows, LANES), 1)

    def columns(q):
        nxt = jnp.where(q == pairs - 1, 0, q + 1)
        odd = tile_of(kern, low_ref[q, 4:8, :], high_ref[pairs - 1 - q, 0:4, :], 1, length)
        even = tile_of(kern, low_ref[nxt, 0:4, :], high_ref[pairs - 1 - nxt, 4:8, :], 0, length)
        here = jnp.where(lane < SUB, 0.0, odd) + jnp.where(lane < LANES - SUB, 0.0, even)
        there = jnp.where(lane < SUB, odd, 0.0) + jnp.where(lane < LANES - SUB, even, 0.0)
        return here, there

    _, there = columns(pairs - 1)
    carry_ref[...] = there

    def step(q, _):
        here, there = columns(q)
        total = here + carry_ref[...]
        carry_ref[...] = there
        for part in range(2):
            value = total[part * tile_rows : (part + 1) * tile_rows]
            at = part * pairs + q
            base = pl.multiple_of(at * row_stride, SUB)
            shared = pl.ds(pl.multiple_of(at * spill, SUB), spill)
            top = value[:spill]
            if not first_band:
                top = top + in_ref[shared, :]
            g_ref[pl.ds(base, spill), :] = top
            g_ref[pl.ds(base + spill, rows - spill), :] = value[spill:rows]
            if not last_band:
                out_ref[shared, :] = value[rows:]
        return 0

    lax.fori_loop(0, pairs, step, 0, unroll=GRID_UNROLL)

    cos = tw_ref[0]
    sin = tw_ref[1]

    def quad(group, _):
        lines = []
        for pair in range(2):
            cells = []
            for one in range(2):
                row = 4 * group + 2 * pair + one
                if last_band:
                    j = row - PATCH - SUB
                    moved = jnp.where(j == 6, 0, jnp.where(j == 7, 7, jnp.where(j % 2 == 0, j + 2, j)))
                    row = jnp.where(is_last & (j >= 0), PATCH + SUB + moved, row)
                cells.append(g_ref[pl.ds(row, parts, stride=row_stride), :])
            hi, lo = split(jnp.concatenate(cells, axis=1))
            out = dot(f1_ref[...], jnp.concatenate([hi, lo], axis=0))
            out = out[:parts] + out[parts:]
            for one in range(2):
                re = out[:pairs, one * LANES : (one + 1) * LANES]
                im = out[pairs:, one * LANES : (one + 1) * LANES]
                lines.append(jnp.concatenate([re * cos - im * sin, re * sin + im * cos], axis=1))
        hi, lo = split(jnp.concatenate(lines, axis=0))
        count = el_ref.shape[0]
        out = dot_nt(eh_ref[...], hi)
        out = out[:count] + out[count:] + dot_nt(el_ref[...], lo)
        dests, _, share, _ = h_ref.shape
        for part in range(2):
            piece = out[:, part * LANES : (part + 1) * LANES].reshape(dests, share, LANES)
            h_ref[:, 2 * group + part, :, :] = piece
        return 0

    lax.fori_loop(0, rows // 4, quad, 0, unroll=QUAD_UNROLL)


GRID_UNROLL = 8
QUAD_UNROLL = 8


def grid_and_rows(last, low, high, kern, tables, carry, dests, length, last_band):
    pairs = low.shape[0]
    spill = 2 * SUB
    rows = PATCH + spill if last_band else PATCH
    row_stride = rows + SUB
    outs = tables[3].shape[0]
    shared = (2 * pairs * spill, LANES)
    vmem = pl.BlockSpec(memory_space=pltpu.VMEM)
    out_shape = [jax.ShapeDtypeStruct((dests, rows * pairs // LANES, outs // dests, LANES), F32)]
    if not last_band:
        out_shape.append(jax.ShapeDtypeStruct(shared, F32))
    args = [low, high, kern, *tables] + ([] if carry is None else [carry])
    out = pl.pallas_call(
        functools.partial(grid_kernel, (pairs, row_stride, length, carry is None, last_band)),
        out_shape=out_shape,
        in_specs=[pl.BlockSpec(memory_space=pltpu.SMEM)] + [vmem] * len(args),
        out_specs=[vmem] * len(out_shape),
        scratch_shapes=[
            pltpu.VMEM((2 * pairs * row_stride, LANES), F32),
            pltpu.VMEM((2 * (PATCH + spill), LANES), F32),
        ],
        compiler_params=pltpu.CompilerParams(vmem_limit_bytes=40 * 1024 * 1024),
        cost_estimate=pl.CostEstimate(flops=20 * 10**9, bytes_accessed=8 * 2**20, transcendentals=0),
        name="grid_rows",
    )(last, *args)
    return out if not last_band else (out[0], None)


def column_kernel(dims, flags_ref, *refs):
    sources, spans, bands, block_rows, vert = dims
    h_refs = refs[:bands]
    f2_ref, f2l_ref, tw_ref, e2_ref, out_ref, r_ref, z_ref, s_ref = refs[bands:]
    share = 2 * spans
    low = flags_ref[0] == 1
    width = LANES
    z_pitch = spans * PATCH + SUB
    half = PATCH // 2

    blocks = sum(ref.shape[1] for ref in h_refs)
    stride = (blocks + 1) * share

    @pl.when(pl.program_id(0) == 0)
    def _():
        def arrived(n, _):
            for i, ref in enumerate(h_refs):
                r_ref[pl.ds(n * (blocks + 1) + i * half, ref.shape[1])] = ref[n]
            return 0

        lax.fori_loop(0, sources, arrived, 0)
        flat = r_ref.reshape(sources * stride, width)
        up_block = SUB // 2 + bands * half
        sub = lax.broadcasted_iota(jnp.int32, (share, width), 0)
        sign = jnp.where(sub % 2 == 0, 1.0, -1.0)

        def at_block(n, block):
            source = jnp.where(low, n, backwards(n, vert, sources // vert))
            return source * (blocks + 1) + block

        def add(to, value):
            r_ref[to] = r_ref[to] + value

        def neighbours(n, _):
            for t in range(SUB // 2):
                add(at_block(n + 1, SUB // 2 + t), r_ref[at_block(n, up_block + t)])
                add(at_block(n, up_block - SUB // 2 + t), r_ref[at_block(n + 1, t)])
            return 0

        lax.fori_loop(0, sources - 1, neighbours, 0)
        for t in range(SUB // 2 - 1):
            add(at_block(sources - 1, up_block - 1 - t), sign * r_ref[at_block(sources - 1, up_block + t)])
        top = r_ref[at_block(sources - 1, up_block + SUB // 2 - 1)]
        lane = lax.broadcasted_iota(jnp.int32, (share, width), 1)
        lifted = jnp.concatenate([top[share - 1 :], top[: share - 1]], axis=0)
        first = at_block(0, SUB // 2)
        r_ref[first] = jnp.where((sub % 2 == 1) & (lane < PATCH), lifted, r_ref[first])

        odd = lax.broadcasted_iota(jnp.int32, (PATCH, width), 1) % 2
        flip = jnp.where(odd == 0, 1.0, -1.0)

        def pair_step(rho, _):
            tall = []
            for k in range(spans):
                cells = []
                for c in range(2):
                    for i in range(bands):
                        row = (SUB // 2 + i * half + rho) * share + 2 * k + c
                        cells.append(flat[pl.ds(row, sources, stride=stride), :])
                tall.append(jnp.concatenate(cells, axis=0).T)
            x = jnp.concatenate(tall, axis=0)
            hi, lo = split(x)
            z = dot(jnp.concatenate([hi, lo], axis=1), f2_ref[...]) + dot(hi, f2l_ref[...])
            top_col = jnp.where(low, x[:, PATCH : PATCH + 1], x[:, PATCH + sources - vert : PATCH + sources - vert + 1])
            for k in range(spans):
                for one in range(2):
                    at = (2 * k + one) * PATCH
                    re = z[at : at + PATCH, :width]
                    im = z[at : at + PATCH, width:]
                    line = 2 * rho + one
                    cos = tw_ref[0, pl.ds(line, 1), :]
                    sin = tw_ref[1, pl.ds(line, 1), :]
                    new_re = re * cos - im * sin
                    new_im = re * sin + im * cos
                    if one == 0:
                        nyquist = flip * top_col[at : at + PATCH]
                        new_im = jnp.where(rho == 0, nyquist, new_im)
                    z_ref[pl.ds(pl.multiple_of(line * z_pitch + k * PATCH, SUB), PATCH), :] = new_re
                    z_ref[pl.ds(pl.multiple_of((PATCH + line) * z_pitch + k * PATCH, SUB), PATCH), :] = new_im
            return 0

        lax.fori_loop(0, half, pair_step, 0, unroll=4)

    start = pl.program_id(0) * block_rows

    def eight(group, _):
        for pair in range(SUB // 2):
            y = start + group * SUB + 2 * pair
            cells = [z_ref[pl.ds(y + one, 2 * PATCH, stride=z_pitch), :] for one in range(2)]
            hi, lo = split(jnp.concatenate(cells, axis=1))
            out = dot(e2_ref[...], jnp.concatenate([hi, lo], axis=0))
            out = out[:PATCH] + out[PATCH:]
            for one in range(2):
                s_ref[pl.ds(2 * pair + one, PATCH, stride=SUB), :] = out[:, one * width : (one + 1) * width]
        at = pl.ds(pl.multiple_of(group * SUB, SUB), SUB)
        for block in range(PATCH):
            out_ref[at, block * width : (block + 1) * width] = s_ref[block * SUB : (block + 1) * SUB, :]
        return 0

    lax.fori_loop(0, block_rows // SUB, eight, 0, unroll=4)


def columns_of(flags, hs, f2, f2l, tw, e2, sources, spans, bands, vert, length):
    y_count = spans * PATCH
    block_rows = min(32, y_count)
    vmem = pl.BlockSpec(memory_space=pltpu.VMEM)
    return pl.pallas_call(
        functools.partial(column_kernel, (sources, spans, bands, block_rows, vert)),
        grid=(y_count // block_rows,),
        out_shape=jax.ShapeDtypeStruct((y_count, length), F32),
        in_specs=[pl.BlockSpec(memory_space=pltpu.SMEM)] + [vmem] * (bands + 4),
        out_specs=pl.BlockSpec((block_rows, length), lambda n: (n, 0)),
        scratch_shapes=[
            pltpu.VMEM((sources * (sum(h.shape[1] for h in hs) + 1), hs[0].shape[2], LANES), F32),
            pltpu.VMEM((2 * PATCH * (y_count + SUB), LANES), F32),
            pltpu.VMEM((PATCH * SUB, LANES), F32),
        ],
        compiler_params=pltpu.CompilerParams(vmem_limit_bytes=46 * 1024 * 1024),
        name="columns",
    )(flags, *hs, f2, f2l, tw, e2)


def split_table(x):
    rounded = lax.reduce_precision(x, 8, 7)
    return rounded.astype(BF16), (x - rounded).astype(BF16)


def stacked(table):
    hi, lo = split_table(table)
    return jnp.concatenate([jnp.concatenate([hi, hi], axis=1), jnp.concatenate([lo, jnp.zeros_like(lo)], axis=1)], axis=0)


def backwards(n, vert, count):
    return (count - 1 - n // vert) * vert + n % vert


def local(vis_value, vis_pos, counts, kernel, *, au, vert):
    devices = au * vert
    half_au = au // 2
    axes = ("half", "sub", "vert")
    me = lax.axis_index(axes)
    low = me < devices // 2
    slots = vis_value.shape[3]
    bands = vis_value.shape[0] // vert
    local_cols = vis_value.shape[1]
    cols = local_cols * vert
    pairs = cols // 2
    length = cols * PATCH
    rows_of_patches = vis_value.shape[0] * au
    scale = 1.0 / math.sqrt(rows_of_patches * cols * slots)
    sources = devices // 2
    y_count = length // devices
    spans = y_count // PATCH

    live = jnp.arange(slots, dtype=jnp.int32) < counts[:, :, None, None]
    fields = jnp.concatenate([jnp.where(live, vis_value, 0.0), vis_pos.astype(F32)], axis=2)
    fields = fields.reshape(vert, bands, local_cols // 2, 8, slots)
    fields = jnp.where(low, fields, fields[::-1, ::-1])
    own, got_first = deal(fields, 2, half_au)
    mirror = [(a * vert + v, (au - 1 - a) * vert + v) for a in range(au) for v in range(vert)]
    received = [got_first[None]]
    if bands > 1:
        later, first_piece = lax.optimization_barrier((own[1:], received[0]))
        received = [first_piece, lax.ppermute(later, axes, mirror)]

    band_index = jnp.where(low, me, lax.axis_index("vert") + vert * (au - 1 - me // vert))
    flags = low.astype(jnp.int32)[None]
    last = (band_index == sources - 1).astype(jnp.int32)[None]

    ya = jnp.arange(pairs, dtype=jnp.int32)
    p = jnp.arange(LANES, dtype=jnp.int32)
    first = real_parts(*turn(ya[:, None] * ya[None, :], pairs))
    f1 = stacked(first.transpose(0, 2, 1, 3).reshape(2 * pairs, 2 * pairs))
    tw1 = jnp.stack(turn(ya[:, None] * p[None, :], length))
    yb = jnp.where(low, 0, LANES // 2) + jnp.arange(LANES // 2, dtype=jnp.int32)
    second = real_parts(*turn(yb[:, None] * p[None, :], LANES))
    second = second.transpose(2, 0, 1, 3).reshape(LANES, 2 * LANES)
    hi, lo = split_table(second)
    tables = (f1, tw1, jnp.concatenate([hi, lo], axis=0), hi)
    carry, hs = None, []
    for band in range(bands):
        got = received[0][0] if band == 0 else received[1][band - 1]
        mine = own if band == 0 else own_later
        low_patches = jnp.where(low, mine[band], got)
        high_patches = jnp.where(low, got, mine[band])
        h, carry = grid_and_rows(
            last, low_patches, high_patches, kernel, tables, carry, sources, length, band == bands - 1
        )
        if band == 0 and bands > 1:
            carry, own_later, received[1] = lax.optimization_barrier((carry, own, received[1]))
        hs.append(lax.all_to_all(h, ("sub", "vert"), split_axis=0, concat_axis=0, tiled=True))

    order = jnp.arange(sources, dtype=jnp.int32)
    order = jnp.where(low, order, backwards(order, vert, half_au))
    d = (bands * order[None, :] + jnp.arange(bands, dtype=jnp.int32)[:, None]).reshape(-1)
    xa = jnp.arange(LANES, dtype=jnp.int32)
    table = real_parts(*turn(xa[:, None] * d[None, :], LANES))
    hi, lo = split_table(table.transpose(1, 3, 0, 2).reshape(2 * PATCH, 2 * LANES))
    r = jnp.arange(PATCH, dtype=jnp.int32)
    tw2 = jnp.stack(turn(r[:, None] * xa[None, :], length))
    cos, sin = turn(r[:, None] * r[None, :], PATCH)
    last = jnp.concatenate([cos, jnp.where(r[None, :] == 0, 1.0, -sin)], axis=1) * scale
    return columns_of(
        flags, hs, jnp.concatenate([hi, hi], axis=0), lo, tw2, stacked(last), sources, spans, bands, vert, length
    )


def solution(mesh):
    au, vert = mesh.shape["au"], mesh.shape["vert"]
    halves = Mesh(mesh.devices.reshape(2, au // 2, vert), ("half", "sub", "vert"))
    rows = ("half", "sub")
    in_specs = (P(rows, "vert", None, None), P(rows, "vert", None, None), P(rows, "vert"), P())

    def program(*args):
        return local(*args, au=au, vert=vert)

    return jax.shard_map(
        program,
        mesh=halves,
        in_specs=in_specs,
        out_specs=P((*rows, "vert"), None),
        check_vma=False,
    )
```
